32 devices in a mesh: grp: 2 (over y), dp: 16 (over z, x, core).
Axes of the slice: x: 2, y: 2, z: 4, core: 2. Of those that a mesh axis runs over, the one named last changes fastest.
Arguments:
- hidden_in: bfloat16 [2, 64, 4096], P(None, ('grp', 'dp')), parts along dimension 1, may hold values from -6 to 6
- norm_gain: float32 [4096], replicated, may hold values from 0.1 to 1.9
- queries: bfloat16 [2, 64, 4096], P(None, ('grp', 'dp')), parts along dimension 1, may hold values from -72 to 72
- new_keys: bfloat16 [2, 64, 1024], P(None, ('grp', 'dp')), parts along dimension 1, may hold values from -9 to 9
- new_values: bfloat16 [2, 64, 1024], P(None, ('grp', 'dp')), parts along dimension 1, may hold values from -6 to 6
- cache_keys: bfloat16 [64, 384, 1024], P(('grp', 'dp')), parts along dimension 0, may hold values from -9 to 9
- cache_values: bfloat16 [64, 384, 1024], P(('grp', 'dp')), parts along dimension 0, may hold values from -6 to 6
- lengths: int32 [64], P(('grp', 'dp')), parts along dimension 0, may hold values from 1 to 384
- routes: int32 [2, 64, 2], P(None, ('grp', 'dp')), parts along dimension 1, may hold values from 0 to 3, all different within a row; in each aligned block of 2 rows (0 to 1, 2 to 3, ..., all dimensions but the last counted through in order) at most 2 rows name the same one
- gate_logits: float32 [2, 64, 2], P(None, ('grp', 'dp')), parts along dimension 1, may hold values from -6 to 6
- w_gate: bfloat16 [28672, 4096], P('dp'), may hold values from -0.09375 to 0.09375
- w_up: bfloat16 [28672, 4096], P('dp'), may hold values from -0.09375 to 0.09375
- w_down: bfloat16 [28672, 4096], P('dp'), may hold values from -0.0625 to 0.0625
Outputs:
- hidden_out: bfloat16 [2, 64, 4096], P(None, ('grp', 'dp')), parts along dimension 1
The draws below stay inside these ranges and needn't reach their ends.
There are 2 independent parts, one for each index of `grp`. The reference program is written for one: setup_inputs(seed, part) draws one part's arguments, and reference() takes and returns one part's arrays. A program takes and returns all parts, laid end to end along the dimension named above; an argument that names none is the same for every part. Nothing has to cross between parts.
Inputs may be any that keep to these rules, and one draw needn't show every extreme that they name: `routes`: each token names 2 different experts. Among the 2 tokens of one device at one decoded position no expert is named more than 2 times, a bound that some block reaches.
All inputs are finite; a program needn't handle non-finite values.
Results may differ from the reference program's by a relative error of at most 0.0055.
Values may be sent and summed in bfloat16 or wider, within the bound.
A program may use at most 192 MiB of HBM per device.

```python
import math
import jax
import jax.numpy as jnp
import numpy as np
from jax import lax

D = 4096
HEADS = 32
KV_HEADS = 8
HEAD_DIM = 128
TOP = 2
EXPERTS = 4
FFW = 7168
NEW = 2
DOC_DEV = 2
CACHE = 384
DOCS = 32
GROUP = 4
KV_WIDTH = 1024
CAP = 2


def key_fields(key):
    cached = jnp.clip(jax.random.normal(jax.random.fold_in(key, 101), (DOCS, CACHE, KV_HEADS * HEAD_DIM), jnp.float32), -5.0, 5.0)
    fresh = jnp.clip(jax.random.normal(jax.random.fold_in(key, 102), (NEW, DOCS, KV_HEADS * HEAD_DIM), jnp.float32), -5.0, 5.0)
    return (cached, fresh)


def draw_cache_keys(key, part):
    cached, fresh = key_fields(key)
    return cached.astype(jnp.bfloat16)


def draw_new_keys(key, part):
    cached, fresh = key_fields(key)
    return fresh.astype(jnp.bfloat16)


def draw_queries(key, part):
    drawn = jnp.clip(jax.random.normal(jax.random.fold_in(key, 104), (NEW, DOCS, HEADS * HEAD_DIM), jnp.float32), -5.0, 5.0)
    return drawn.astype(jnp.bfloat16)


def touch_ends(values, own_key, low, high):
    shape = values.shape
    index_at = [jax.random.randint(jax.random.fold_in(own_key, axis), (), 0, shape[axis]) for axis in range(len(shape))]
    values = values.at[tuple(index_at)].set(low)
    longest = shape.index(max(shape))
    index_at[longest] = (index_at[longest] + 1) % shape[longest]
    return values.at[tuple(index_at)].set(high)


def steps_of(key, extent, shards, low, top_value):
    def one(axis_at, parts):
        steps = jax.random.uniform(jax.random.fold_in(jax.random.fold_in(key, 6), axis_at), (parts,), jnp.float32, low / len(shards), top_value / len(shards))
        return jnp.repeat(jnp.exp(steps), extent[axis_at] // parts).reshape((-1,) + (1,) * (len(extent) - axis_at - 1))

    loudness = one(*shards[0])
    for cut in shards[1:]:
        loudness = loudness * one(*cut)
    return loudness


def routed_block(own_key, own, number, rows, amount, top, most, lean):
    sequence = jax.random.permutation(own_key, amount)
    crowded, common = load_shares(amount, rows * top, most, lean, True), load_shares(amount, rows * top, most, lean, False)
    places = jnp.arange(amount)

    def named(sizes, turn):
        used = int((sizes > 0).sum())
        fixed = max(1, used // 4)
        passed = fixed + (places - fixed + turn * (used - fixed)) % max(1, amount - fixed)
        return jnp.zeros((amount,), jnp.int32).at[sequence[jnp.where(places < fixed, places, passed)]].set(jnp.asarray(sizes, jnp.int32))

    sizes = jnp.where(number % 4 == 0, named(crowded, number // 4), named(common, number - number // 4 - 1))
    mixed = jax.random.permutation(jax.random.fold_in(own, 3), amount)
    source_of, taker = mixed[0:amount // 2 * 2:2], mixed[1:amount // 2 * 2:2]
    margin = jnp.minimum(sizes[source_of] - 1, most - sizes[taker]) // 2
    margin = jnp.where((source_of == sequence[0]) | (taker == sequence[0]) | (sizes[taker] == 0), 0, jnp.maximum(margin, 0))
    passed = jax.random.randint(jax.random.fold_in(own, 4), (amount // 2,), 0, 1 << 20) % (margin + 1)
    sizes = sizes.at[source_of].add(-passed).at[taker].add(passed)
    labels = jnp.searchsorted(jnp.cumsum(sizes), jnp.arange(rows * top), side="right").astype(jnp.int32)
    table = labels.reshape(top, rows).T
    table = table[jax.random.permutation(jax.random.fold_in(own, 1), rows)]
    turn = jax.random.randint(jax.random.fold_in(own, 2), (rows, 1), 0, top)
    return jnp.take_along_axis(table, (jnp.arange(top)[None, :] + turn) % top, axis=1)


def load_shares(amount, total, limit, lean, full):
    weights = [(1 << 20) // math.isqrt(grade ** lean) + 1 for grade in range(1, amount + 1)]
    largest = limit if full else min(limit, max(-(-total // amount), total * weights[0] // sum(weights)))
    least = 1 if total - largest >= amount - 1 else 0
    holding, spare = [largest] + [least] * (amount - 1), total - largest - least * (amount - 1)
    while spare > 0:
        free = [i for i in range(1, amount) if holding[i] < largest] or [i for i in range(1, amount) if holding[i] < limit]
        whole, budget = sum([weights[i] for i in free]), spare
        for i in free:
            more = min(limit - holding[i], max(1, budget * weights[i] // whole), spare)
            holding[i] = holding[i] + more
            spare = spare - more
    return np.array(holding)


def gaussian(key, dims, scale, most, shards=(), kind=jnp.bfloat16):
    values = jax.random.normal(key, dims, jnp.float32) * scale
    if len(shards) > 0:
        values = steps_of(key, dims, shards, -0.22, 0.18) * values
    return jnp.clip(values, min=-most, max=most).astype(kind)


def setup_inputs(seed: int = 0, part: int = 0) -> dict:
    arg_keys = jax.random.split(jax.random.key(seed), 14)
    part_keys = jax.random.split(jax.random.fold_in(arg_keys[13], part), 14)
    hidden_in = gaussian(part_keys[0], (NEW, DOCS, D), 1.0, 6.0, ((1, 16),))
    norm_gain = jnp.clip(1.0 + 0.18 * jax.random.normal(arg_keys[1], (D,), jnp.float32), 0.1, 1.9)
    queries = draw_queries(jax.random.fold_in(jax.random.fold_in(arg_keys[13], part), 71), part)
    new_keys = draw_new_keys(jax.random.fold_in(jax.random.fold_in(arg_keys[13], part), 71), part)
    new_values = gaussian(part_keys[4], (NEW, DOCS, KV_WIDTH), 1.0, 6.0, ((1, 16),))
    cache_keys = draw_cache_keys(jax.random.fold_in(jax.random.fold_in(arg_keys[13], part), 71), part)
    cache_values = gaussian(part_keys[6], (DOCS, CACHE, KV_WIDTH), 1.0, 6.0, ((0, 16),))
    lengths = touch_ends(jax.random.randint(part_keys[7], (DOCS,), 1, CACHE + 1), jax.random.fold_in(part_keys[7], 1), 1, CACHE).astype(jnp.int32)
    routes_keys = jax.random.split(jax.random.fold_in(part_keys[8], 1), NEW * DOCS // DOC_DEV)
    routes_turns = jax.random.permutation(jax.random.fold_in(part_keys[8], 3), NEW * DOCS // DOC_DEV)
    routes = jax.vmap(lambda own, number: routed_block(jax.random.fold_in(part_keys[8], 2), own, number, DOC_DEV, EXPERTS, TOP, CAP, 2))(routes_keys, routes_turns).reshape((NEW, DOCS, TOP))
    gate_logits = gaussian(part_keys[9], (NEW, DOCS, TOP), 1.5, 6.0, ((1, 16),), jnp.float32)
    w_gate = gaussian(arg_keys[10], (EXPERTS * FFW, D), D ** -0.5, 0.09375, ((0, 16),))
    w_up = gaussian(arg_keys[11], (EXPERTS * FFW, D), D ** -0.5, 0.09375, ((0, 16),))
    w_down = gaussian(arg_keys[12], (EXPERTS * FFW, D), FFW ** -0.5, 0.0625, ((0, 16),))
    return {"hidden_in": hidden_in, "norm_gain": norm_gain, "queries": queries, "new_keys": new_keys, "new_values": new_values, "cache_keys": cache_keys, "cache_values": cache_values, "lengths": lengths, "routes": routes, "gate_logits": gate_logits, "w_gate": w_gate, "w_up": w_up, "w_down": w_down}


def attend(queries, new_keys, new_values, cache_keys, cache_values, lengths):
    docs = queries.shape[1]
    cache_len = cache_keys.shape[1]
    score_scale = HEAD_DIM ** (-0.5)
    query_heads = queries.astype(jnp.float32).reshape(NEW, docs, KV_HEADS, GROUP, HEAD_DIM)
    keys_cache = cache_keys.astype(jnp.float32).reshape(docs, cache_len, KV_HEADS, HEAD_DIM)
    vals_cache = cache_values.astype(jnp.float32).reshape(docs, cache_len, KV_HEADS, HEAD_DIM)
    keys_fresh = new_keys.astype(jnp.float32).reshape(NEW, docs, KV_HEADS, HEAD_DIM)
    vals_fresh = new_values.astype(jnp.float32).reshape(NEW, docs, KV_HEADS, HEAD_DIM)
    scores_cache = jnp.einsum('tdhgc,dshc->tdhgs', query_heads, keys_cache) * score_scale
    scores_fresh = jnp.einsum('tdhgc,udhc->tdhgu', query_heads, keys_fresh) * score_scale
    positions = jnp.arange(cache_len, dtype=jnp.int32)
    in_range = positions[None, :] < lengths[:, None]
    scores_cache = jnp.where(in_range[None, :, None, None, :], scores_cache, -1e+30)
    order = jnp.arange(NEW, dtype=jnp.int32)
    causal = order[None, :] <= order[:, None]
    scores_fresh = jnp.where(causal[:, None, None, None, :], scores_fresh, -1e+30)
    largest = jnp.maximum(lax.optimization_barrier(jnp.max(scores_cache, -1, keepdims=True)), lax.optimization_barrier(jnp.max(scores_fresh, -1, keepdims=True)))
    exp_cache = jnp.exp(scores_cache - largest)
    exp_fresh = jnp.exp(scores_fresh - largest)
    total = lax.optimization_barrier(jnp.sum(exp_cache, -1, keepdims=True)) + lax.optimization_barrier(jnp.sum(exp_fresh, -1, keepdims=True))
    probs_cache = (exp_cache / total).astype(jnp.bfloat16).astype(jnp.float32)
    probs_fresh = (exp_fresh / total).astype(jnp.bfloat16).astype(jnp.float32)
    context = jnp.einsum('tdhgs,dshc->tdhgc', probs_cache, vals_cache)
    context = context + jnp.einsum('tdhgu,udhc->tdhgc', probs_fresh, vals_fresh)
    return context.reshape(NEW, docs, HEADS * HEAD_DIM)

def reference(hidden_in, norm_gain, queries, new_keys, new_values, cache_keys, cache_values, lengths, routes, gate_logits, w_gate, w_up, w_down):
    context = attend(queries, new_keys, new_values, cache_keys, cache_values, lengths)
    carried = hidden_in.astype(jnp.float32) + context
    normed = (carried * lax.rsqrt(lax.optimization_barrier(jnp.mean(carried * carried, -1, keepdims=True)) + 1e-05) * norm_gain).astype(jnp.bfloat16)
    flat_rows = normed.reshape(NEW * DOCS, D)
    flat_routes = routes.reshape(NEW * DOCS, TOP)
    flat_logits = gate_logits.reshape(NEW * DOCS, TOP)
    top_share = jax.nn.sigmoid(flat_logits[:, 0] - flat_logits[:, 1])
    shares = jnp.stack([top_share, 1.0 - top_share], axis=1)
    result = carried.reshape(NEW * DOCS, D)
    for expert in range(EXPERTS):
        weight_rows = lax.optimization_barrier(jnp.sum(shares * (flat_routes == expert).astype(jnp.float32), axis=1))
        gate_block = w_gate[expert * FFW:(expert + 1) * FFW]
        up_block = w_up[expert * FFW:(expert + 1) * FFW]
        down_block = w_down[expert * FFW:(expert + 1) * FFW]
        gate_val = lax.dot_general(flat_rows, gate_block, (((1,), (1,)), ((), ())), preferred_element_type=jnp.float32)
        up_val = lax.dot_general(flat_rows, up_block, (((1,), (1,)), ((), ())), preferred_element_type=jnp.float32)
        act = (jax.nn.silu(gate_val) * up_val).astype(jnp.bfloat16)
        expert_out = jnp.dot(act, down_block, preferred_element_type=jnp.float32)
        result = result + weight_rows[:, None] * expert_out
    return result.reshape(NEW, DOCS, D).astype(jnp.bfloat16)
```

```python
import functools

import jax
import jax.numpy as jnp
from jax import lax
from jax.experimental import pallas as pl
from jax.experimental.pallas import tpu as pltpu
from jax.sharding import PartitionSpec as P

HEAD_DIM = 128
EXPERTS = 4
MESH = pl.DeviceIdType.MESH
F32 = jnp.float32
BF16 = jnp.bfloat16


def kernel(
    n,
    hc,
    cw,
    lengths_ref,
    routes_ref,
    logits_ref,
    hidden_ref,
    gain_ref,
    q_ref,
    nk_ref,
    nv_ref,
    ck_hbm,
    cv_hbm,
    wg_hbm,
    wu_hbm,
    wd_hbm,
    out_ref,
    kbuf,
    vbuf,
    wg,
    wu,
    wd,
    qs,
    ctx,
    carried,
    blocks,
    xs,
    xb,
    act,
    part,
    s1,
    r1,
    s2,
    r2,
    s3,
    r3,
    sem_kv,
    sem_gu,
    sem_d,
    sem_a,
    sem_b,
    sem_c,
    sem_1,
    sem_2,
    sem_3,
):
    new, docs, width = hidden_ref.shape
    tokens = new * docs
    cache_len, kv_width = ck_hbm.shape[1], ck_hbm.shape[2]
    kv_heads = kv_width // HEAD_DIM
    group = width // kv_width
    rows8 = new * group
    hidden = wg_hbm.shape[0]
    nj = hidden // hc
    nk = width // cw
    quads = n // 4
    rows = n * tokens
    score_scale = HEAD_DIM ** (-0.5)

    grp, me = lax.axis_index("grp"), lax.axis_index("dp")
    core = lax.rem(me, 2)
    xbit = lax.rem(me // 2, 2)
    quad = me // 4
    core_dev = (grp, me + 1 - 2 * core)
    x_dev = (grp, me + 2 - 4 * xbit)

    def quad_dev(d):
        return (grp, lax.rem(quad + d, quads) * 4 + lax.rem(me, 4))

    barrier = pltpu.get_barrier_semaphore()
    for dev in [core_dev, x_dev] + [quad_dev(d) for d in range(1, quads)]:
        pl.semaphore_signal(barrier, inc=1, device_id=dev, device_id_type=MESH)

    k_copies = [
        pltpu.make_async_copy(ck_hbm.at[d], kbuf.at[d], sem_kv.at[0, d]) for d in range(docs)
    ]
    v_copies = [
        pltpu.make_async_copy(cv_hbm.at[d], vbuf.at[d], sem_kv.at[1, d]) for d in range(docs)
    ]
    for copy in k_copies + v_copies:
        copy.start()

    def gate_copy(j):
        return pltpu.make_async_copy(wg_hbm.at[pl.ds(j * hc, hc)], wg.at[j], sem_gu.at[0, j])

    def up_copy(j):
        return pltpu.make_async_copy(wu_hbm.at[pl.ds(j * hc, hc)], wu.at[j], sem_gu.at[1, j])

    def down_copy(k):
        return pltpu.make_async_copy(wd_hbm.at[:, pl.ds(k * cw, cw)], wd.at[k], sem_d.at[k])

    for j in range(nj):
        gate_copy(j).start()
        up_copy(j).start()
    for k in range(nk):
        down_copy(k).start()

    for t in range(new):
        q32 = q_ref[t].astype(F32)
        for d in range(docs):
            for head in range(kv_heads * group):
                h, g = head // group, head % group
                r = t * group + g
                qs[d * kv_heads + h, r : r + 1, :] = q32[
                    d : d + 1, head * HEAD_DIM : (head + 1) * HEAD_DIM
                ]
    nk32 = [nk_ref[u].astype(F32) for u in range(new)]
    nv32 = [nv_ref[u].astype(F32) for u in range(new)]
    row_pos = lax.broadcasted_iota(jnp.int32, (rows8, 1), 0) // group
    col = lax.broadcasted_iota(jnp.int32, (rows8, cache_len), 1)
    for d in range(docs):
        k_copies[d].wait()
        v_copies[d].wait()
        keep = col < lengths_ref[d]
        for h in range(kv_heads):
            lanes = slice(h * HEAD_DIM, (h + 1) * HEAD_DIM)
            q8 = qs[d * kv_heads + h]
            scores = lax.dot_general(
                q8.astype(BF16),
                kbuf[d, :, lanes],
                (((1,), (1,)), ((), ())),
                preferred_element_type=F32,
            )
            scores = jnp.where(keep, scores * score_scale, -1e30)
            fresh = []
            for u in range(new):
                s = jnp.sum(q8 * nk32[u][d : d + 1, lanes], axis=1, keepdims=True) * score_scale
                fresh.append(jnp.where(row_pos >= u, s, -1e30))
            largest = jnp.max(scores, axis=1, keepdims=True)
            for s in fresh:
                largest = jnp.maximum(largest, s)
            e = jnp.exp(scores - largest)
            ef = [jnp.exp(s - largest) for s in fresh]
            total = jnp.sum(e, axis=1, keepdims=True)
            for x in ef:
                total = total + x
            c8 = jnp.dot(
                (e / total).astype(BF16), vbuf[d, :, lanes], preferred_element_type=F32
            )
            for u in range(new):
                c8 = c8 + (ef[u] / total).astype(BF16).astype(F32) * nv32[u][d : d + 1, lanes]
            for t in range(new):
                for g in range(group):
                    r = t * group + g
                    head = h * group + g
                    ctx[t * docs + d : t * docs + d + 1, head * HEAD_DIM : (head + 1) * HEAD_DIM] = c8[
                        r : r + 1
                    ]
    for t in range(new):
        carried[t * docs : (t + 1) * docs, :] = (
            hidden_ref[t].astype(F32) + ctx[t * docs : (t + 1) * docs, :]
        )
    car = carried[...]
    mean = jnp.mean(car * car, axis=1, keepdims=True)
    blocks[me] = (car * lax.rsqrt(mean + 1e-05) * gain_ref[...]).astype(BF16)

    pl.semaphore_wait(barrier, quads + 1)

    def block_copy(index, send_sem, recv_sem, dev):
        return pltpu.make_async_remote_copy(
            src_ref=blocks.at[index],
            dst_ref=blocks.at[index],
            send_sem=send_sem,
            recv_sem=recv_sem,
            device_id=dev,
            device_id_type=MESH,
        )

    inner = lax.rem(me, 4)

    def place(d, y, c):
        return lax.rem(quad + quads - d, quads) * 4 + lax.rem(xbit + y, 2) * 2 + lax.rem(core + c, 2)

    out_a = [
        block_copy(me, sem_a.at[0, d], sem_a.at[1, d], quad_dev(d)) for d in range(1, quads)
    ]
    out_b = [
        block_copy(place(d, 0, 0), sem_b.at[0, d], sem_b.at[1, d], x_dev) for d in range(quads)
    ]
    out_c = [
        [
            block_copy(place(d, y, 0), sem_c.at[0, y, d], sem_c.at[1, y, d], core_dev)
            for y in range(2)
        ]
        for d in range(quads)
    ]
    in_a = [None] + [
        block_copy(place(d, 0, 0), sem_a.at[0, d], sem_a.at[1, d], core_dev)
        for d in range(1, quads)
    ]
    in_b = [
        block_copy(place(d, 1, 0), sem_b.at[0, d], sem_b.at[1, d], x_dev) for d in range(quads)
    ]
    in_c = [
        [
            block_copy(place(d, y, 1), sem_c.at[0, y, d], sem_c.at[1, y, d], core_dev)
            for y in range(2)
        ]
        for d in range(quads)
    ]
    for copy in out_a:
        copy.start()
    order = [0] + [d for i in range(1, quads // 2 + 1) for d in dict.fromkeys([i, quads - i])]
    for d in order:
        if d > 0:
            in_a[d].wait_recv()
        out_b[d].start()
        out_c[d][0].start()
    for d in order:
        in_b[d].wait_recv()
        out_c[d][1].start()
    for d in order:
        for y in range(2):
            in_c[d][y].wait_recv()
    for b in range(n):
        xs[b * tokens : (b + 1) * tokens, :] = blocks[b].astype(F32)
    xb[...] = xs[...].astype(BF16)

    def hidden_step(j):
        gate_copy(j).wait()
        up_copy(j).wait()
        x = xb[...]
        dims = (((1,), (1,)), ((), ()))
        gate = lax.dot_general(x, wg[j], dims, preferred_element_type=F32)
        up = lax.dot_general(x, wu[j], dims, preferred_element_type=F32)
        return (gate * jax.nn.sigmoid(gate) * up).astype(BF16)

    if nj == 1:
        act[...] = hidden_step(0)
    else:

        def body(j, carry):
            act[:, pl.ds(pl.multiple_of(j * hc, hc), hc)] = hidden_step(j)
            return carry

        lax.fori_loop(0, nj, body, 0)

    def pair_copy(src, dst, sems, dev):
        return pltpu.make_async_remote_copy(
            src_ref=src,
            dst_ref=dst,
            send_sem=sems.at[0],
            recv_sem=sems.at[1],
            device_id=dev,
            device_id_type=MESH,
        )

    copy_1 = [
        pair_copy(s1.at[k, 1 - core], r1.at[k], sem_1.at[k], core_dev) for k in range(nk)
    ]
    copy_2 = [pair_copy(s2.at[k, 1 - xbit], r2.at[k], sem_2.at[k], x_dev) for k in range(nk)]
    copy_3 = [
        [
            pair_copy(
                s3.at[k, lax.rem(quad + d, quads)], r3.at[k, quad], sem_3.at[k, d], quad_dev(d)
            )
            for d in range(1, quads)
        ]
        for k in range(nk)
    ]
    wait_3 = [
        [
            pair_copy(
                s3.at[k, lax.rem(quad + d, quads)],
                r3.at[k, lax.rem(quad + quads - d, quads)],
                sem_3.at[k, d],
                quad_dev(d),
            )
            for d in range(1, quads)
        ]
        for k in range(nk)
    ]

    def start_1(k):
        down_copy(k).wait()
        part[...] = jnp.dot(act[...], wd[k], preferred_element_type=F32)
        for b in range(n):
            s1[k, b % 2, b // 2] = part[b * tokens : (b + 1) * tokens, :].astype(BF16)
        copy_1[k].start()

    def start_2(k):
        copy_1[k].wait_recv()
        for q in range(quads):
            for y in range(2):
                h = q * 2 + y
                s2[k, y, q] = (s1[k, core, h].astype(F32) + r1[k, h].astype(F32)).astype(BF16)
        copy_2[k].start()

    def start_3(k):
        copy_2[k].wait_recv()
        for q in range(quads):
            s3[k, q] = (s2[k, xbit, q].astype(F32) + r2[k, q].astype(F32)).astype(BF16)
        r3[k, quad] = s3[k, quad]
        for copy in copy_3[k]:
            copy.start()

    token = lax.broadcasted_iota(jnp.int32, (tokens, 1), 0)
    margin = jnp.zeros((tokens, 1), F32)
    first = jnp.zeros((tokens, 1), jnp.int32)
    second = jnp.zeros((tokens, 1), jnp.int32)
    for t in range(new):
        for d in range(docs):
            here = token == t * docs + d
            margin = jnp.where(here, logits_ref[t, d, 0] - logits_ref[t, d, 1], margin)
            first = jnp.where(here, routes_ref[t, d, 0], first)
            second = jnp.where(here, routes_ref[t, d, 1], second)
    share_a = jax.nn.sigmoid(margin)
    share_b = 1.0 - share_a
    share = [
        jnp.where(first == e, share_a, 0.0) + jnp.where(second == e, share_b, 0.0)
        for e in range(EXPERTS)
    ]

    def finish(k):
        for copy in wait_3[k]:
            copy.wait_recv()
        lanes = slice(k * cw, (k + 1) * cw)
        acc = carried[:, lanes]
        for e in range(EXPERTS):
            per = quads // EXPERTS
            value = r3[k, e * per].astype(F32)
            for i in range(1, per):
                value = value + r3[k, e * per + i].astype(F32)
            acc = acc + share[e] * value
        for t in range(new):
            out_ref[t, :, lanes] = acc[t * docs : (t + 1) * docs].astype(out_ref.dtype)

    for step in range(nk + 3):
        if step < nk:
            start_1(step)
        if 0 <= step - 1 < nk:
            start_2(step - 1)
        if 0 <= step - 2 < nk:
            start_3(step - 2)
        if 0 <= step - 3 < nk:
            finish(step - 3)

    for copy in out_a + out_b + [c for pair in out_c for c in pair]:
        copy.wait_send()
    for k in range(nk):
        copy_1[k].wait_send()
        copy_2[k].wait_send()
        for copy in copy_3[k]:
            copy.wait_send()


def hidden_chunk(hidden):
    for size in range(256, 0, -16):
        if hidden % size == 0 and (size % 128 == 0 or size == hidden):
            return size
    return hidden


def per_device(
    hidden_in,
    norm_gain,
    queries,
    new_keys,
    new_values,
    cache_keys,
    cache_values,
    lengths,
    routes,
    gate_logits,
    w_gate,
    w_up,
    w_down,
):
    n = lax.axis_size("dp")
    new, docs, width = hidden_in.shape
    tokens = new * docs
    rows = n * tokens
    hidden = w_gate.shape[0]
    cache_len, kv_width = cache_keys.shape[1:]
    kv_heads = kv_width // HEAD_DIM
    hc = hidden_chunk(hidden)
    nj = hidden // hc
    nk = 4
    cw = width // nk
    quads = n // 4
    smem = pl.BlockSpec(memory_space=pltpu.SMEM)
    vmem = pl.BlockSpec(memory_space=pltpu.VMEM)
    hbm = pl.BlockSpec(memory_space=pl.ANY)
    dma = pltpu.SemaphoreType.DMA
    return pl.pallas_call(
        functools.partial(kernel, n, hc, cw),
        out_shape=jax.ShapeDtypeStruct(hidden_in.shape, BF16),
        in_specs=[smem] * 3 + [vmem] * 5 + [hbm] * 5,
        out_specs=vmem,
        scratch_shapes=[
            pltpu.VMEM(cache_keys.shape, BF16),
            pltpu.VMEM(cache_values.shape, BF16),
            pltpu.VMEM((nj, hc, width), BF16),
            pltpu.VMEM((nj, hc, width), BF16),
            pltpu.VMEM((nk, hidden, cw), BF16),
            pltpu.VMEM((docs * kv_heads, new * width // kv_width, HEAD_DIM), F32),
            pltpu.VMEM((tokens, width), F32),
            pltpu.VMEM((tokens, width), F32),
            pltpu.VMEM((n, tokens, width), BF16),
            pltpu.VMEM((rows, width), F32),
            pltpu.VMEM((rows, width), BF16),
            pltpu.VMEM((rows, hidden), BF16),
            pltpu.VMEM((rows, cw), F32),
            pltpu.VMEM((nk, 2, n // 2, tokens, cw), BF16),
            pltpu.VMEM((nk, n // 2, tokens, cw), BF16),
            pltpu.VMEM((nk, 2, quads, tokens, cw), BF16),
            pltpu.VMEM((nk, quads, tokens, cw), BF16),
            pltpu.VMEM((nk, quads, tokens, cw), BF16),
            pltpu.VMEM((nk, quads, tokens, cw), BF16),
            dma((2, docs)),
            dma((2, nj)),
            dma((nk,)),
            dma((2, quads)),
            dma((2, quads)),
            dma((2, 2, quads)),
            dma((nk, 2)),
            dma((nk, 2)),
            dma((nk, quads, 2)),
        ],
        compiler_params=pltpu.CompilerParams(
            collective_id=0, has_side_effects=True, vmem_limit_bytes=67043328
        ),
        name="decode_layer",
    )(
        lengths,
        routes,
        gate_logits,
        hidden_in,
        norm_gain.reshape(1, width),
        queries,
        new_keys,
        new_values,
        cache_keys,
        cache_values,
        w_gate,
        w_up,
        w_down,
    )


def solution(mesh):
    in_specs = (
        P(None, ("grp", "dp"), None),
        P(),
        P(None, ("grp", "dp"), None),
        P(None, ("grp", "dp"), None),
        P(None, ("grp", "dp"), None),
        P(("grp", "dp"), None, None),
        P(("grp", "dp"), None, None),
        P(("grp", "dp")),
        P(None, ("grp", "dp"), None),
        P(None, ("grp", "dp"), None),
        P("dp", None),
        P("dp", None),
        P("dp", None),
    )
    out_specs = P(None, ("grp", "dp"), None)
    return jax.shard_map(
        per_device, mesh=mesh, in_specs=in_specs, out_specs=out_specs, check_vma=False
    )
```

```python
import functools

import jax
import jax.numpy as jnp
from jax import lax
from jax.experimental import pallas as pl
from jax.experimental.pallas import tpu as pltpu
from jax.sharding import PartitionSpec as P

HEAD_DIM = 128
EXPERTS = 4
MESH = pl.DeviceIdType.MESH
F32 = jnp.float32
BF16 = jnp.bfloat16


def kernel(
    n,
    hc,
    cw,
    lengths_ref,
    routes_ref,
    logits_ref,
    hidden_ref,
    gain_ref,
    q_ref,
    nk_ref,
    nv_ref,
    ck_hbm,
    cv_hbm,
    wg_hbm,
    wu_hbm,
    wd_hbm,
    out_ref,
    kbuf,
    vbuf,
    wg,
    wu,
    wd,
    qs,
    ctx,
    carried,
    blocks,
    xs,
    xb,
    act,
    part,
    s1,
    r1,
    s2,
    r2,
    s3,
    r3,
    sem_kv,
    sem_gu,
    sem_d,
    sem_a,
    sem_b,
    sem_c,
    sem_1,
    sem_2,
    sem_3,
):
    new, docs, width = hidden_ref.shape
    tokens = new * docs
    cache_len, kv_width = ck_hbm.shape[1], ck_hbm.shape[2]
    kv_heads = kv_width // HEAD_DIM
    group = width // kv_width
    rows8 = new * group
    hidden = wg_hbm.shape[0]
    nj = hidden // hc
    nk = width // cw
    quads = n // 4
    rows = n * tokens
    score_scale = HEAD_DIM ** (-0.5)

    grp, me = lax.axis_index("grp"), lax.axis_index("dp")
    core = lax.rem(me, 2)
    xbit = lax.rem(me // 2, 2)
    quad = me // 4
    core_dev = (grp, me + 1 - 2 * core)
    x_dev = (grp, me + 2 - 4 * xbit)

    def quad_dev(d):
        return (grp, lax.rem(quad + d, quads) * 4 + lax.rem(me, 4))

    barrier = pltpu.get_barrier_semaphore()
    for dev in [core_dev, x_dev] + [quad_dev(d) for d in range(1, quads)]:
        pl.semaphore_signal(barrier, inc=1, device_id=dev, device_id_type=MESH)

    k_copies = [
        pltpu.make_async_copy(ck_hbm.at[d], kbuf.at[d], sem_kv.at[0, d]) for d in range(docs)
    ]
    v_copies = [
        pltpu.make_async_copy(cv_hbm.at[d], vbuf.at[d], sem_kv.at[1, d]) for d in range(docs)
    ]
    for copy in k_copies + v_copies:
        copy.start()

    def gate_copy(j):
        return pltpu.make_async_copy(wg_hbm.at[pl.ds(j * hc, hc)], wg.at[j], sem_gu.at[0, j])

    def up_copy(j):
        return pltpu.make_async_copy(wu_hbm.at[pl.ds(j * hc, hc)], wu.at[j], sem_gu.at[1, j])

    def down_copy(k):
        return pltpu.make_async_copy(wd_hbm.at[:, pl.ds(k * cw, cw)], wd.at[k], sem_d.at[k])

    for t in range(new):
        q32 = q_ref[t].astype(F32)
        for d in range(docs):
            for head in range(kv_heads * group):
                h, g = head // group, head % group
                r = t * group + g
                qs[d * kv_heads + h, r : r + 1, :] = q32[
                    d : d + 1, head * HEAD_DIM : (head + 1) * HEAD_DIM
                ]
    nk32 = [nk_ref[u].astype(F32) for u in range(new)]
    nv32 = [nv_ref[u].astype(F32) for u in range(new)]
    row_pos = lax.broadcasted_iota(jnp.int32, (rows8, 1), 0) // group
    col = lax.broadcasted_iota(jnp.int32, (rows8, cache_len), 1)
    for copy in k_copies + v_copies:
        copy.wait()
    for j in range(nj):
        gate_copy(j).start()
        up_copy(j).start()
    for k in range(nk):
        down_copy(k).start()
    for d in range(docs):
        keep = col < lengths_ref[d]
        for h in range(kv_heads):
            lanes = slice(h * HEAD_DIM, (h + 1) * HEAD_DIM)
            q8 = qs[d * kv_heads + h]
            scores = lax.dot_general(
                q8.astype(BF16),
                kbuf[d, :, lanes],
                (((1,), (1,)), ((), ())),
                preferred_element_type=F32,
            )
            scores = jnp.where(keep, scores * score_scale, -1e30)
            fresh = []
            for u in range(new):
                s = jnp.sum(q8 * nk32[u][d : d + 1, lanes], axis=1, keepdims=True) * score_scale
                fresh.append(jnp.where(row_pos >= u, s, -1e30))
            largest = jnp.max(scores, axis=1, keepdims=True)
            for s in fresh:
                largest = jnp.maximum(largest, s)
            e = jnp.exp(scores - largest)
            ef = [jnp.exp(s - largest) for s in fresh]
            total = jnp.sum(e, axis=1, keepdims=True)
            for x in ef:
                total = total + x
            c8 = jnp.dot(
                (e / total).astype(BF16), vbuf[d, :, lanes], preferred_element_type=F32
            )
            for u in range(new):
                c8 = c8 + (ef[u] / total).astype(BF16).astype(F32) * nv32[u][d : d + 1, lanes]
            for t in range(new):
                for g in range(group):
                    r = t * group + g
                    head = h * group + g
                    ctx[t * docs + d : t * docs + d + 1, head * HEAD_DIM : (head + 1) * HEAD_DIM] = c8[
                        r : r + 1
                    ]
    for t in range(new):
        carried[t * docs : (t + 1) * docs, :] = (
            hidden_ref[t].astype(F32) + ctx[t * docs : (t + 1) * docs, :]
        )
    car = carried[...]
    mean = jnp.mean(car * car, axis=1, keepdims=True)
    blocks[me] = (car * lax.rsqrt(mean + 1e-05) * gain_ref[...]).astype(BF16)

    pl.semaphore_wait(barrier, quads + 1)

    def block_copy(index, send_sem, recv_sem, dev):
        return pltpu.make_async_remote_copy(
            src_ref=blocks.at[index],
            dst_ref=blocks.at[index],
            send_sem=send_sem,
            recv_sem=recv_sem,
            device_id=dev,
            device_id_type=MESH,
        )

    inner = lax.rem(me, 4)

    def place(d, y, c):
        return lax.rem(quad + quads - d, quads) * 4 + lax.rem(xbit + y, 2) * 2 + lax.rem(core + c, 2)

    out_a = [
        block_copy(me, sem_a.at[0, d], sem_a.at[1, d], quad_dev(d)) for d in range(1, quads)
    ]
    out_b = [
        block_copy(place(d, 0, 0), sem_b.at[0, d], sem_b.at[1, d], x_dev) for d in range(quads)
    ]
    out_c = [
        [
            block_copy(place(d, y, 0), sem_c.at[0, y, d], sem_c.at[1, y, d], core_dev)
            for y in range(2)
        ]
        for d in range(quads)
    ]
    in_a = [None] + [
        block_copy(place(d, 0, 0), sem_a.at[0, d], sem_a.at[1, d], core_dev)
        for d in range(1, quads)
    ]
    in_b = [
        block_copy(place(d, 1, 0), sem_b.at[0, d], sem_b.at[1, d], x_dev) for d in range(quads)
    ]
    in_c = [
        [
            block_copy(place(d, y, 1), sem_c.at[0, y, d], sem_c.at[1, y, d], core_dev)
            for y in range(2)
        ]
        for d in range(quads)
    ]
    for copy in out_a:
        copy.start()
    order = [0] + [d for i in range(1, quads // 2 + 1) for d in dict.fromkeys([i, quads - i])]
    for d in order:
        if d > 0:
            in_a[d].wait_recv()
        out_b[d].start()
        out_c[d][0].start()
    for d in order:
        in_b[d].wait_recv()
        out_c[d][1].start()
    for d in order:
        for y in range(2):
            in_c[d][y].wait_recv()
    for b in range(n):
        xs[b * tokens : (b + 1) * tokens, :] = blocks[b].astype(F32)
    xb[...] = xs[...].astype(BF16)

    def hidden_step(j):
        gate_copy(j).wait()
        up_copy(j).wait()
        x = xb[...]
        dims = (((1,), (1,)), ((), ()))
        gate = lax.dot_general(x, wg[j], dims, preferred_element_type=F32)
        up = lax.dot_general(x, wu[j], dims, preferred_element_type=F32)
        return (gate * jax.nn.sigmoid(gate) * up).astype(BF16)

    if nj == 1:
        act[...] = hidden_step(0)
    else:

        def body(j, carry):
            act[:, pl.ds(pl.multiple_of(j * hc, hc), hc)] = hidden_step(j)
            return carry

        lax.fori_loop(0, nj, body, 0)

    def pair_copy(src, dst, sems, dev):
        return pltpu.make_async_remote_copy(
            src_ref=src,
            dst_ref=dst,
            send_sem=sems.at[0],
            recv_sem=sems.at[1],
            device_id=dev,
            device_id_type=MESH,
        )

    copy_1 = [
        pair_copy(s1.at[k, 1 - core], r1.at[k], sem_1.at[k], core_dev) for k in range(nk)
    ]
    copy_2 = [pair_copy(s2.at[k, 1 - xbit], r2.at[k], sem_2.at[k], x_dev) for k in range(nk)]
    copy_3 = [
        [
            pair_copy(
                s3.at[k, lax.rem(quad + d, quads)], r3.at[k, quad], sem_3.at[k, d], quad_dev(d)
            )
            for d in range(1, quads)
        ]
        for k in range(nk)
    ]
    wait_3 = [
        [
            pair_copy(
                s3.at[k, lax.rem(quad + d, quads)],
                r3.at[k, lax.rem(quad + quads - d, quads)],
                sem_3.at[k, d],
                quad_dev(d),
            )
            for d in range(1, quads)
        ]
        for k in range(nk)
    ]

    def start_1(k):
        down_copy(k).wait()
        part[...] = jnp.dot(act[...], wd[k], preferred_element_type=F32)
        for b in range(n):
            s1[k, b % 2, b // 2] = part[b * tokens : (b + 1) * tokens, :].astype(BF16)
        copy_1[k].start()

    def start_2(k):
        copy_1[k].wait_recv()
        for q in range(quads):
            for y in range(2):
                h = q * 2 + y
                s2[k, y, q] = (s1[k, core, h].astype(F32) + r1[k, h].astype(F32)).astype(BF16)
        copy_2[k].start()

    def start_3(k):
        copy_2[k].wait_recv()
        for q in range(quads):
            s3[k, q] = (s2[k, xbit, q].astype(F32) + r2[k, q].astype(F32)).astype(BF16)
        r3[k, quad] = s3[k, quad]
        for copy in copy_3[k]:
            copy.start()

    token = lax.broadcasted_iota(jnp.int32, (tokens, 1), 0)
    margin = jnp.zeros((tokens, 1), F32)
    first = jnp.zeros((tokens, 1), jnp.int32)
    second = jnp.zeros((tokens, 1), jnp.int32)
    for t in range(new):
        for d in range(docs):
            here = token == t * docs + d
            margin = jnp.where(here, logits_ref[t, d, 0] - logits_ref[t, d, 1], margin)
            first = jnp.where(here, routes_ref[t, d, 0], first)
            second = jnp.where(here, routes_ref[t, d, 1], second)
    share_a = jax.nn.sigmoid(margin)
    share_b = 1.0 - share_a
    share = [
        jnp.where(first == e, share_a, 0.0) + jnp.where(second == e, share_b, 0.0)
        for e in range(EXPERTS)
    ]

    def finish(k):
        for copy in wait_3[k]:
            copy.wait_recv()
        lanes = slice(k * cw, (k + 1) * cw)
        acc = carried[:, lanes]
        for e in range(EXPERTS):
            per = quads // EXPERTS
            value = r3[k, e * per].astype(F32)
            for i in range(1, per):
                value = value + r3[k, e * per + i].astype(F32)
            acc = acc + share[e] * value
        for t in range(new):
            out_ref[t, :, lanes] = acc[t * docs : (t + 1) * docs].astype(out_ref.dtype)

    for step in range(nk + 3):
        if step < nk:
            start_1(step)
        if 0 <= step - 1 < nk:
            start_2(step - 1)
        if 0 <= step - 2 < nk:
            start_3(step - 2)
        if 0 <= step - 3 < nk:
            finish(step - 3)

    for copy in out_a + out_b + [c for pair in out_c for c in pair]:
        copy.wait_send()
    for k in range(nk):
        copy_1[k].wait_send()
        copy_2[k].wait_send()
        for copy in copy_3[k]:
            copy.wait_send()


def hidden_chunk(hidden):
    for size in range(256, 0, -16):
        if hidden % size == 0 and (size % 128 == 0 or size == hidden):
            return size
    return hidden


def per_device(
    hidden_in,
    norm_gain,
    queries,
    new_keys,
    new_values,
    cache_keys,
    cache_values,
    lengths,
    routes,
    gate_logits,
    w_gate,
    w_up,
    w_down,
):
    n = lax.axis_size("dp")
    new, docs, width = hidden_in.shape
    tokens = new * docs
    rows = n * tokens
    hidden = w_gate.shape[0]
    cache_len, kv_width = cache_keys.shape[1:]
    kv_heads = kv_width // HEAD_DIM
    hc = hidden_chunk(hidden)
    nj = hidden // hc
    nk = 2
    cw = width // nk
    quads = n // 4
    smem = pl.BlockSpec(memory_space=pltpu.SMEM)
    vmem = pl.BlockSpec(memory_space=pltpu.VMEM)
    hbm = pl.BlockSpec(memory_space=pl.ANY)
    dma = pltpu.SemaphoreType.DMA
    return pl.pallas_call(
        functools.partial(kernel, n, hc, cw),
        out_shape=jax.ShapeDtypeStruct(hidden_in.shape, BF16),
        in_specs=[smem] * 3 + [vmem] * 5 + [hbm] * 5,
        out_specs=vmem,
        scratch_shapes=[
            pltpu.VMEM(cache_keys.shape, BF16),
            pltpu.VMEM(cache_values.shape, BF16),
            pltpu.VMEM((nj, hc, width), BF16),
            pltpu.VMEM((nj, hc, width), BF16),
            pltpu.VMEM((nk, hidden, cw), BF16),
            pltpu.VMEM((docs * kv_heads, new * width // kv_width, HEAD_DIM), F32),
            pltpu.VMEM((tokens, width), F32),
            pltpu.VMEM((tokens, width), F32),
            pltpu.VMEM((n, tokens, width), BF16),
            pltpu.VMEM((rows, width), F32),
            pltpu.VMEM((rows, width), BF16),
            pltpu.VMEM((rows, hidden), BF16),
            pltpu.VMEM((rows, cw), F32),
            pltpu.VMEM((nk, 2, n // 2, tokens, cw), BF16),
            pltpu.VMEM((nk, n // 2, tokens, cw), BF16),
            pltpu.VMEM((nk, 2, quads, tokens, cw), BF16),
            pltpu.VMEM((nk, quads, tokens, cw), BF16),
            pltpu.VMEM((nk, quads, tokens, cw), BF16),
            pltpu.VMEM((nk, quads, tokens, cw), BF16),
            dma((2, docs)),
            dma((2, nj)),
            dma((nk,)),
            dma((2, quads)),
            dma((2, quads)),
            dma((2, 2, quads)),
            dma((nk, 2)),
            dma((nk, 2)),
            dma((nk, quads, 2)),
        ],
        compiler_params=pltpu.CompilerParams(
            collective_id=0, has_side_effects=True, vmem_limit_bytes=67043328
        ),
        name="decode_layer",
    )(
        lengths,
        routes,
        gate_logits,
        hidden_in,
        norm_gain.reshape(1, width),
        queries,
        new_keys,
        new_values,
        cache_keys,
        cache_values,
        w_gate,
        w_up,
        w_down,
    )


def solution(mesh):
    in_specs = (
        P(None, ("grp", "dp"), None),
        P(),
        P(None, ("grp", "dp"), None),
        P(None, ("grp", "dp"), None),
        P(None, ("grp", "dp"), None),
        P(("grp", "dp"), None, None),
        P(("grp", "dp"), None, None),
        P(("grp", "dp")),
        P(None, ("grp", "dp"), None),
        P(None, ("grp", "dp"), None),
        P("dp", None),
        P("dp", None),
        P("dp", None),
    )
    out_specs = P(None, ("grp", "dp"), None)
    return jax.shard_map(
        per_device, mesh=mesh, in_specs=in_specs, out_specs=out_specs, check_vma=False
    )
```
